256 devices in a mesh: coil: 8 (over y, core), spoke: 32 (over x, z).
Axes of the slice: x: 4, y: 4, z: 8, core: 2. Of those that a mesh axis runs over, the one named last changes fastest.
Arguments:
- kdata: bfloat16 [256, 16, 2, 64, 256], P('spoke', 'coil'), may hold values from -6 to 6
- coords: float32 [256, 2, 256], P('spoke'), may hold values from 0 to 256, as said below
- foot_offset: int32 [256, 32], P('spoke'), may hold values from 0 to 224, as said below
- live_count: int32 [32], P('spoke'), may hold values from 1 to 8, 192 in all
- dcf_table: float32 [129], replicated, may hold values from 0.1 to 4
- dcf_index: int32 [256, 256], P('spoke'), may hold values from 0 to 128
- slab_owner: int32 [32], replicated, may hold values from 0 to 31, each once
Outputs:
- coil_images: float32 [256, 16, 2, 64, 256], P('spoke', 'coil')
- combined: float32 [256, 64, 256], P('spoke', 'coil')
The draws below stay inside these ranges and needn't reach their ends.
Inputs may be any that keep to these rules, and one draw needn't show every extreme that they name: coords[p, 0, s] lies between s and s + 1; coords[p, 1, s] lies between foot_offset[p, s // 8] + 3 and foot_offset[p, s // 8] + 29. `foot_offset`: for each block of 8 spoke slots (the slots of one device index of spoke) and each slab, the offsets lie between b and b + 16, where b is the smallest of them, and both ends are taken; b <= 208.
All inputs are finite; a program needn't handle non-finite values. No bound on the sum of `live_count` on one device may be relied on, other than what follows from the above.
Results may differ from the reference program's by a relative error of at most 0.0028.
Values may be sent and summed in bfloat16 or wider, within the bound.
A program may use at most 128 MiB of HBM per device.

```python
import math
import jax
import jax.numpy as jnp
import numpy as np
from jax import lax

GRID = 256
KZ = 64
S_DEV = 8
FW = 32
UW = 48
HALO = 4
COILS = 16
SPOKES = 256
SAMP = 256
NW = 129
N_SPOKE = 32


def footprint_layout(key):
    slab_rows = GRID // N_SPOKE
    slope_key, relative_key, pick_key = jax.random.split(jax.random.fold_in(key, 71), 3)
    slopes = jax.random.randint(slope_key, (N_SPOKE,), -64, 65)
    centres = jnp.arange(N_SPOKE, dtype=jnp.int32) * slab_rows + slab_rows // 2 - GRID // 2
    window_base = GRID // 2 + centres[None, :] * slopes[:, None] // 64 - UW // 2
    window_base = jnp.clip(window_base, 0, GRID - UW)
    relative = jax.random.randint(relative_key, (N_SPOKE, S_DEV, N_SPOKE), 0, UW - FW + 1)
    shuffled = jax.vmap(lambda subkey: jax.random.permutation(subkey, S_DEV))(jax.random.split(pick_key, N_SPOKE))
    low_slot = shuffled[:, 0]
    high_slot = shuffled[:, 1]
    slot_ids = jnp.arange(S_DEV, dtype=jnp.int32)
    relative = jnp.where(slot_ids[None, :, None] == low_slot[:, None, None], 0, relative)
    relative = jnp.where(slot_ids[None, :, None] == high_slot[:, None, None], UW - FW, relative)
    layout = window_base[:, None, :] + relative
    return layout.reshape(N_SPOKE * S_DEV, N_SPOKE).astype(jnp.int32)


def draw_foot_offset(key, part):
    return footprint_layout(key)


def draw_coords(key, part):
    offsets = footprint_layout(key)
    slab_rows = GRID // N_SPOKE
    first_key, second_key = jax.random.split(jax.random.fold_in(key, 5))
    sample = jnp.arange(GRID, dtype=jnp.int32)
    reach = FW // 2 - 3
    along = jax.random.uniform(first_key, (SPOKES, GRID), jnp.float32, -0.5, 0.5)
    across = jax.random.uniform(second_key, (SPOKES, GRID), jnp.float32, -reach, reach)
    row_coord = sample.astype(jnp.float32)[None, :] + 0.5 + along
    start_cols = offsets[:, sample // slab_rows].astype(jnp.float32)
    col_coord = start_cols + FW / 2 + across
    return jnp.stack([row_coord, col_coord], axis=1).astype(jnp.float32)


def draw_dcf_index(key, part):
    sample = jnp.arange(GRID, dtype=jnp.int32)
    radial = jnp.abs(2 * sample + 1 - GRID) // 2
    jitter = jax.random.randint(jax.random.fold_in(key, 13), (SPOKES, GRID), 0, 2)
    return jnp.minimum(radial[None, :] + jitter, NW - 1).astype(jnp.int32)


def steps_of(stream_key, extent, cuts, smallest, high):
    level, own = 1.0, jax.random.fold_in(stream_key, 6)
    for axis_at, shards_of in cuts:
        heights = jnp.exp(jax.random.uniform(jax.random.fold_in(own, axis_at), (shards_of,), jnp.float32, smallest / len(cuts), high / len(cuts)))
        level = level * jnp.repeat(heights, extent[axis_at] // shards_of).reshape([-1 if axis == axis_at else 1 for axis in range(len(extent))])
    return level


def profile(amount, total, most, slope):
    loads = [(1 << 20) // math.isqrt(rank ** slope) + 1 for rank in range(2, amount + 1)]
    rest, holding = total - most - (amount - 1), [1] * (amount - 1)
    while rest > 0:
        movable = [i for i in range(amount - 1) if holding[i] < most]
        pool, remaining = sum([loads[i] for i in movable]), rest
        for i in movable:
            more = min(most - holding[i], max(1, remaining * loads[i] // pool), rest)
            holding[i] = holding[i] + more
            rest = rest - more
    return np.array([most] + holding)


def uneven(own_key, count, total, most, slope):
    if count == 2:
        one = jax.random.randint(own_key, (), max(1, total - most), min(most, total - 1) + 1)
        return jnp.stack([one, total - one])
    sizes = jnp.asarray(profile(count, total, most, slope), jnp.int32)
    couples = (count - 1) // 2
    source_of, taker = sizes[1:1 + 2 * couples:2], sizes[2:2 + 2 * couples:2]
    slack = jnp.minimum(source_of - 1, most - taker)
    passed = jax.random.randint(jax.random.fold_in(own_key, 1), (couples,), 0, 1 << 20) % (slack + 1)
    sizes = sizes.at[1:1 + 2 * couples:2].set(source_of - passed).at[2:2 + 2 * couples:2].set(taker + passed)
    return sizes[jax.random.permutation(jax.random.fold_in(own_key, 2), count)]


def normal_values(stream_key, shape, deviation, most, shards=(), held_as=jnp.bfloat16):
    drawn = jax.random.normal(stream_key, shape, jnp.float32) * deviation
    if len(shards) > 0:
        drawn = steps_of(stream_key, shape, shards, -0.22, 0.18) * drawn
    return jnp.clip(drawn, min=-most, max=most).astype(held_as)


def setup_inputs(seed: int = 0) -> dict:
    arg_keys = jax.random.split(jax.random.key(seed), 8)
    return {
        "kdata": normal_values(arg_keys[0], (SPOKES, COILS, 2, KZ, SAMP), 1.0, 6.0, ((0, 32), (1, 8))),
        "coords": draw_coords(jax.random.fold_in(arg_keys[7], 71), 0),
        "foot_offset": draw_foot_offset(jax.random.fold_in(arg_keys[7], 71), 0),
        "live_count": uneven(arg_keys[3], N_SPOKE, (3 * S_DEV * N_SPOKE) // 4, S_DEV, 2).astype(jnp.int32),
        "dcf_table": jnp.clip(jnp.exp(jax.random.uniform(arg_keys[4], (NW,), jnp.float32, math.log(0.1), math.log(4.0))), 0.1, 4.0),
        "dcf_index": draw_dcf_index(jax.random.fold_in(arg_keys[7], 71), 0),
        "slab_owner": jax.random.permutation(arg_keys[6], N_SPOKE).astype(jnp.int32),
    }


def kernel(distance):
    inner = jnp.maximum(1.0 - distance * distance * 0.25, 0.0)
    return inner * inner

def reference(kdata, coords, foot_offset, live_count, dcf_table, dcf_index, slab_owner):
    spokes = kdata.shape[0]
    slab_rows = GRID // N_SPOKE
    block_len = slab_rows + 2 * HALO
    columns = COILS * 2 * KZ
    slot_index = jnp.arange(spokes, dtype=jnp.int32)
    live_flag = (slot_index % S_DEV < jnp.repeat(live_count, S_DEV)).astype(jnp.float32)
    density = dcf_table[dcf_index] * live_flag[:, None]
    values = kdata.reshape(spokes, columns, SAMP)

    def one_slab(slab_index):
        position = (slab_index * slab_rows - HALO + jnp.arange(block_len, dtype=jnp.int32)).astype(jnp.int32)
        inside = (position >= 0) & (position < SAMP)
        clipped = jnp.clip(position, 0, SAMP - 1).astype(jnp.int32)
        row_coord = coords[:, 0, :][:, clipped]
        col_coord = coords[:, 1, :][:, clipped]
        block_density = jnp.where(inside[None, :], density[:, clipped], 0.0)
        sample_block = jnp.where(inside[None, None, :], values[:, :, clipped], jnp.zeros((), kdata.dtype)).astype(jnp.float32)
        rows = (slab_index * slab_rows + jnp.arange(slab_rows, dtype=jnp.int32)).astype(jnp.float32)
        row_weight = block_density[:, :, None] * kernel(rows[None, None, :] + 0.5 - row_coord[:, :, None])
        offsets = jnp.take(foot_offset, slab_index, axis=1).astype(jnp.int32)
        cell_cols = offsets[:, None] + jnp.arange(FW, dtype=jnp.int32)[None, :]
        col_weight = kernel(cell_cols.astype(jnp.float32)[:, None, :] + 0.5 - col_coord[:, :, None])
        weights = (row_weight[..., None] * col_weight[:, :, None, :]).astype(jnp.bfloat16)
        weights = lax.optimization_barrier(weights).astype(jnp.float32)
        weights = weights.reshape(N_SPOKE, S_DEV, block_len, slab_rows * FW)
        grouped = sample_block.reshape(N_SPOKE, S_DEV, columns, block_len)
        cell_groups = cell_cols.reshape(N_SPOKE, S_DEV, FW)

        def add_group(running, group_data):
            group_values, group_weights, cell_index = group_data
            tile_sums = jnp.einsum('pcq,pqk->cpk', group_values, group_weights)
            tile_sums = tile_sums.reshape(columns, S_DEV, slab_rows, FW).transpose(0, 2, 1, 3)
            return (running.at[:, :, cell_index].add(tile_sums), None)
        start = jnp.zeros((columns, slab_rows, GRID), jnp.float32)
        slab_grid, _ = lax.scan(add_group, start, (grouped, weights, cell_groups))
        layered = slab_grid.reshape(COILS, 2, KZ, slab_rows, GRID)
        spectrum = layered[:, 0] + 1j * layered[:, 1]
        image = jnp.fft.ifft2(spectrum, axes=(1, 3), norm='ortho')
        images = jnp.stack([jnp.real(image), jnp.imag(image)], axis=1).astype(jnp.float32)
        images = images.transpose(3, 0, 1, 2, 4)
        power_sum = lax.optimization_barrier(jnp.sum(images * images, axis=(1, 2)))
        return (images, power_sum)
    all_images, all_power = lax.map(one_slab, jnp.arange(N_SPOKE, dtype=jnp.int32))
    coil_images = all_images[slab_owner].reshape(GRID, COILS, 2, KZ, GRID)
    combined = jnp.sqrt(all_power[slab_owner]).reshape(GRID, KZ, GRID)
    return (coil_images, combined)
```

```python
import math

import jax
import jax.numpy as jnp
import numpy as np
from jax import lax
from jax.experimental import pallas as pl
from jax.experimental.pallas import tpu as pltpu
from jax.sharding import PartitionSpec as P

MESH = pl.DeviceIdType.MESH
FW = 32
REACH = 2
COIL_DEV = 8
SPOKE_DEV = 32
X_DEV = 4
Z_DEV = 8
SLOTS = 8
ROWS = 8
BLOCK = ROWS + 2 * REACH
PAIRS = BLOCK // 2
COLS = 128
GROUPS = 4
PER = SPOKE_DEV // GROUPS
BAND = 3 * 16 * PER
F32 = jnp.float32
BF16 = jnp.bfloat16


def kernel(distance):
    inner = jnp.maximum(1.0 - distance * distance * 0.25, 0.0)
    return inner * inner


def depth_table(length):
    phase = 2.0 * np.pi / length * (np.outer(np.arange(length), np.arange(length)) % length)
    c, s = np.cos(phase) / math.sqrt(length), np.sin(phase) / math.sqrt(length)
    return np.block([[c, -s], [s, c]])


def column_table(length):
    phase = 2.0 * np.pi / length * (np.outer(np.arange(length), np.arange(length)) % length)
    return np.concatenate([np.cos(phase), np.sin(phase)], axis=1) / math.sqrt(length)


def thirds(x):
    high = x.astype(BF16)
    rest = x - high.astype(F32)
    mid = rest.astype(BF16)
    low = (rest - mid.astype(F32)).astype(BF16)
    return high, mid, low


def dot_nt(a, b):
    return lax.dot_general(a, b, (((1,), (1,)), ((), ())), preferred_element_type=F32)


def dot(a, b):
    return jnp.dot(a, b, preferred_element_type=F32)


def body(
    owner_ref, live_ref, kdata_hbm, select_ref, place_ref, coords_ref, foot_ref, table_ref, index_ref, depth_ref, column_ref,
    images_hbm, combined_ref,
    kd, stage, send, recv, geo_send, geo, weights, fold, grid, images, power, power_send, power_recv,
    kd_sem, geo_ssem, geo_rsem, pass_ssem, pass_rsem, val_ssem, val_rsem, pow_ssem, pow_rsem, out_sem,
):
    me = lax.axis_index("spoke")
    coil = lax.axis_index("coil")
    x, z = me // Z_DEV, lax.rem(me, Z_DEV)

    def away(slot, sign):
        r = lax.rem(slot, Z_DEV)
        odd = lax.rem(r, 2)
        dz = lax.rem(odd * ((r + 1) // 2) + (1 - odd) * (Z_DEV - r // 2), Z_DEV)
        dx = slot // Z_DEV
        return lax.rem(x + sign * dx + X_DEV, X_DEV) * Z_DEV + lax.rem(z + sign * dz + Z_DEV, Z_DEV)

    load = pltpu.make_async_copy(kdata_hbm, kd, kd_sem)
    load.start()

    barrier = pltpu.get_barrier_semaphore()

    @pl.loop(1, SPOKE_DEV)
    def _(slot):
        pl.semaphore_signal(barrier, inc=1, device_id=(coil, away(slot, 1)), device_id_type=MESH)

    @pl.loop(1, COIL_DEV)
    def _(step):
        pl.semaphore_signal(barrier, inc=1, device_id=(lax.rem(coil + step, COIL_DEV), me), device_id_type=MESH)

    row_of = lax.broadcasted_iota(jnp.int32, (8, 256), 0)
    lane_of = lax.broadcasted_iota(jnp.int32, (8, 256), 1)
    high, mid, low = thirds(jnp.broadcast_to(table_ref[...], (8, 256)))
    table3 = jnp.where(
        row_of == 0,
        high.astype(F32),
        jnp.where(row_of == 1, mid.astype(F32), jnp.where(row_of == 2, low.astype(F32), 0.0)),
    ).astype(BF16)
    entry = lax.broadcasted_iota(jnp.int32, (256, 256), 0)
    density = jnp.zeros((8, 256), F32)
    for p in range(SLOTS):
        hit = jnp.where(entry == index_ref[p : p + 1, :], 1.0, 0.0).astype(BF16)
        looked = jnp.sum(dot(table3, hit), axis=0, keepdims=True)
        density = density + jnp.where(row_of == p, looked, 0.0)
    density = jnp.where(row_of < live_ref[0], density, 0.0)
    parts = []
    for comp in (coords_ref[0], coords_ref[1], density, foot_ref[...]):
        parts.extend(t.astype(F32) for t in thirds(comp))
    geometry = jnp.concatenate(parts, axis=0).astype(BF16)
    sample = lax.broadcasted_iota(jnp.int32, (256, 128), 0)
    group_of = lax.broadcasted_iota(jnp.int32, (8, 128), 1) // 32
    for t in range(GROUPS):
        dest = away(t * 8 + coil, 1)
        hit = jnp.where(sample == place_ref[pl.ds(dest, 1), :], 1.0, 0.0).astype(BF16)
        got = dot(geometry, hit)
        tile = jnp.zeros((8, 128), F32)
        for c in range(4):
            part = got[24 * c : 24 * c + 8] + got[24 * c + 8 : 24 * c + 16] + got[24 * c + 16 : 24 * c + 24]
            tile = jnp.where(group_of == c, part, tile)
        geo_send[t] = tile

    def fill(c):
        for p in range(SLOTS):
            stage[pl.ds(p, SPOKE_DEV * BLOCK, stride=SLOTS), :] = dot_nt(
                select_ref[...], kd[p, c * COLS : (c + 1) * COLS, :]
            )
        send[c] = stage[...].astype(BF16).reshape(SPOKE_DEV, BLOCK * SLOTS, COLS)

    load.wait()
    fill(0)

    pl.semaphore_wait(barrier, SPOKE_DEV - 1 + COIL_DEV - 1)

    def geo_copy(t):
        return pltpu.make_async_remote_copy(
            geo_send.at[t],
            geo.at[coil, t],
            geo_ssem.at[t],
            geo_rsem.at[t],
            device_id=(coil, away(t * 8 + coil, 1)),
            device_id_type=MESH,
        )

    def value_copy(c, slot):
        dest = away(slot, 1)
        return pltpu.make_async_remote_copy(
            send.at[c, dest],
            recv.at[c, slot],
            val_ssem.at[c, slot],
            val_rsem.at[c, slot],
            device_id=(coil, dest),
            device_id_type=MESH,
        )

    def pass_copy(step):
        return pltpu.make_async_remote_copy(
            geo.at[coil],
            geo.at[coil],
            pass_ssem.at[step],
            pass_rsem.at[step],
            device_id=(lax.rem(coil + step, COIL_DEV), me),
            device_id_type=MESH,
        )

    def pass_arrival(step):
        source = lax.rem(coil - step + COIL_DEV, COIL_DEV)
        return pltpu.make_async_remote_copy(
            geo.at[source],
            geo.at[source],
            pass_ssem.at[step],
            pass_rsem.at[step],
            device_id=(lax.rem(coil + step, COIL_DEV), me),
            device_id_type=MESH,
        )

    for t in range(1, GROUPS):
        geo_copy(t).start()

    @pl.when(coil != 0)
    def _():
        geo_copy(0).start()

    @pl.when(coil == 0)
    def _():
        geo[0, 0] = geo_send[0]

    @pl.loop(1, SPOKE_DEV)
    def _(slot):
        value_copy(0, slot).start()

    fill(1)

    @pl.loop(1, SPOKE_DEV)
    def _(slot):
        value_copy(1, slot).start()

    recv[0, 0] = send[0, me]
    recv[1, 0] = send[1, me]

    for t in range(1, GROUPS):
        geo_copy(t).wait_recv()

    @pl.when(coil != 0)
    def _():
        geo_copy(0).wait_recv()

    @pl.loop(1, COIL_DEV)
    def _(step):
        pass_copy(step).start()

    @pl.loop(1, COIL_DEV)
    def _(step):
        pass_arrival(step).wait_recv()

    first_row = (owner_ref[me] * ROWS).astype(F32)
    cells = lax.broadcasted_iota(jnp.int32, (8, 256), 1).astype(F32)

    @pl.loop(0, SPOKE_DEV)
    def _(slot):
        group = slot // PER
        member = lax.rem(slot, PER)
        tile = geo[lax.rem(slot, 8), slot // 8]

        def spread(comp, j):
            lane = comp * 32 + j
            return jnp.broadcast_to(tile[:, lane : lane + 1], (8, 256))

        across, along = [], []
        for j in range(BLOCK):
            start = spread(3, j)
            covered = (cells >= start) & (cells < start + FW)
            across.append(jnp.where(covered, kernel(cells + 0.5 - spread(1, j)), 0.0))
            along.append((spread(0, j)[:, :128], spread(2, j)[:, :128]))
        at = pl.multiple_of(member * 16, 16)
        for g in range(ROWS):
            for i in range(3):
                pair = []
                for j in (2 * (g // 2 + i), 2 * (g // 2 + i) + 1):
                    row, dens = along[j]
                    value = dens * kernel(first_row + (g + 0.5) - row)
                    pair.append(jnp.concatenate([value, value], axis=1) * across[j])
                weights[group, g, pl.ds(i * 16 * PER + at, 16), :] = jnp.concatenate(pair, axis=0).astype(BF16)

    for c in range(2):
        for q in range(GROUPS):

            @pl.loop(max(1, q * PER), (q + 1) * PER)
            def _(slot):
                value_copy(c, slot).wait_recv()

            for i in range(PAIRS):
                got = recv[c, q * PER : (q + 1) * PER, i * 16 : (i + 1) * 16, :].reshape(16 * PER, COLS)
                folded = dot_nt(depth_ref[0], got) + dot_nt(depth_ref[1], got)
                fold[:, i * 16 * PER : (i + 1) * 16 * PER] = folded.astype(BF16)
            for g in range(ROWS):
                at = (g // 2) * 16 * PER
                term = dot(fold[:, at : at + BAND], weights[q, g])
                grid[g] = term if q == 0 else grid[g] + term
        for h in range(ROWS // 2):
            pair = []
            for g in (2 * h, 2 * h + 1):
                turned = dot(grid[g].astype(BF16), column_ref[...])
                real = turned[:64, :256] - turned[64:, 256:]
                imag = turned[:64, 256:] + turned[64:, :256]
                images[g, c, 0] = real
                images[g, c, 1] = imag
                mine = real * real + imag * imag
                if c == 0:
                    power[g] = mine
                else:
                    pair.append(power[g] + mine)
            out = pltpu.make_async_copy(
                images.at[pl.ds(2 * h, 2), c], images_hbm.at[pl.ds(2 * h, 2), c], out_sem.at[c, h]
            )
            out.start()
            if c == 1:
                for k in range(COIL_DEV):
                    power_send[h, k] = jnp.concatenate([m[8 * k : 8 * k + 8] for m in pair], axis=0).astype(BF16)

                @pl.loop(1, COIL_DEV)
                def _(step):
                    power_copy(power_send, power_recv, pow_ssem, pow_rsem, coil, me, h, step).start()

    for h in range(ROWS // 2):
        power_recv[h, 0] = power_send[h, coil]

        @pl.loop(1, COIL_DEV)
        def _(step):
            power_copy(power_send, power_recv, pow_ssem, pow_rsem, coil, me, h, step).wait_recv()

        total = power_recv[h, 0].astype(F32)
        for k in range(1, COIL_DEV):
            total = total + power_recv[h, k].astype(F32)
        combined = jnp.sqrt(total)
        combined_ref[2 * h] = combined[:8]
        combined_ref[2 * h + 1] = combined[8:]

    for c in range(2):
        for h in range(ROWS // 2):
            pltpu.make_async_copy(
                images.at[pl.ds(2 * h, 2), c], images_hbm.at[pl.ds(2 * h, 2), c], out_sem.at[c, h]
            ).wait()

        @pl.loop(1, SPOKE_DEV)
        def _(slot):
            value_copy(c, slot).wait_send()

    for t in range(1, GROUPS):
        geo_copy(t).wait_send()

    @pl.when(coil != 0)
    def _():
        geo_copy(0).wait_send()

    @pl.loop(1, COIL_DEV)
    def _(step):
        pass_copy(step).wait_send()
        for h in range(ROWS // 2):
            power_copy(power_send, power_recv, pow_ssem, pow_rsem, coil, me, h, step).wait_send()


def power_copy(power_send, power_recv, ssem, rsem, coil, me, h, step):
    peer = lax.rem(coil + step, COIL_DEV)
    return pltpu.make_async_remote_copy(
        power_send.at[h, peer],
        power_recv.at[h, step],
        ssem.at[h, step],
        rsem.at[h, step],
        device_id=(peer, me),
        device_id_type=MESH,
    )


def on_device(kdata, coords, foot_offset, live_count, dcf_table, dcf_index, slab_owner):
    slots, coil_dev, parts, kz, samp = kdata.shape
    kd = kdata.reshape(slots, coil_dev * parts * kz, samp)
    first = slab_owner * ROWS - REACH
    wanted = (first[:, None] + jnp.arange(BLOCK, dtype=jnp.int32)[None, :]).reshape(-1)
    select = (wanted[:, None] == jnp.arange(samp, dtype=jnp.int32)[None, :]).astype(BF16)
    lane = jnp.arange(128, dtype=jnp.int32)[None, :]
    place = jnp.where(
        lane >= 96,
        slab_owner[:, None],
        jnp.where(lane % 32 < BLOCK, first[:, None] + lane % 32, -1),
    )
    table = jnp.pad(dcf_table, (0, 256 - dcf_table.shape[0])).reshape(1, 256)
    foot = jnp.pad(foot_offset.astype(F32), ((0, 0), (0, 256 - foot_offset.shape[1])))
    exact = depth_table(kz)
    coarse = np.asarray(exact, BF16)
    depth = jnp.asarray(np.stack([coarse, np.asarray(exact - coarse.astype(np.float64), BF16)]))
    column = jnp.asarray(column_table(samp), BF16)
    vmem = pl.BlockSpec(memory_space=pltpu.VMEM)
    smem = pl.BlockSpec(memory_space=pltpu.SMEM)
    hbm = pl.BlockSpec(memory_space=pl.ANY)
    dma = pltpu.SemaphoreType.DMA
    images, combined = pl.pallas_call(
        body,
        out_shape=(
            jax.ShapeDtypeStruct((ROWS, coil_dev, parts, kz, samp), F32),
            jax.ShapeDtypeStruct((ROWS, kz // COIL_DEV, samp), F32),
        ),
        in_specs=[smem, smem, hbm] + [vmem] * 8,
        out_specs=(hbm, vmem),
        scratch_shapes=[
            pltpu.VMEM((slots, coil_dev * parts * kz, samp), BF16),
            pltpu.VMEM((SPOKE_DEV * BLOCK * SLOTS, COLS), F32),
            pltpu.VMEM((2, SPOKE_DEV, BLOCK * SLOTS, COLS), BF16),
            pltpu.VMEM((2, SPOKE_DEV, BLOCK * SLOTS, COLS), BF16),
            pltpu.VMEM((GROUPS, 8, 128), F32),
            pltpu.VMEM((COIL_DEV, GROUPS, 8, 128), F32),
            pltpu.VMEM((GROUPS, ROWS, BAND, 256), BF16),
            pltpu.VMEM((COLS, PAIRS * 16 * PER), BF16),
            pltpu.VMEM((ROWS, COLS, 256), F32),
            pltpu.VMEM((ROWS, coil_dev, parts, kz, samp), F32),
            pltpu.VMEM((ROWS, kz, samp), F32),
            pltpu.VMEM((ROWS // 2, COIL_DEV, 16, samp), BF16),
            pltpu.VMEM((ROWS // 2, COIL_DEV, 16, samp), BF16),
            dma,
            dma((GROUPS,)),
            dma((GROUPS,)),
            dma((COIL_DEV,)),
            dma((COIL_DEV,)),
            dma((2, SPOKE_DEV)),
            dma((2, SPOKE_DEV)),
            dma((ROWS // 2, COIL_DEV)),
            dma((ROWS // 2, COIL_DEV)),
            dma((2, ROWS // 2)),
        ],
        compiler_params=pltpu.CompilerParams(
            collective_id=0, has_side_effects=True, vmem_limit_bytes=56 * 2**20
        ),
    )(
        slab_owner,
        live_count,
        kd,
        select,
        place,
        jnp.transpose(coords, (1, 0, 2)),
        foot,
        table,
        dcf_index,
        depth,
        column,
    )
    return images, combined


def solution(mesh):
    return jax.shard_map(
        on_device,
        mesh=mesh,
        in_specs=(
            P("spoke", "coil", None, None, None),
            P("spoke", None, None),
            P("spoke", None),
            P("spoke"),
            P(),
            P("spoke", None),
            P(),
        ),
        out_specs=(P("spoke", "coil", None, None, None), P("spoke", "coil", None)),
        check_vma=False,
    )
```

```python
import math

import jax
import jax.numpy as jnp
import numpy as np
from jax import lax
from jax.experimental import pallas as pl
from jax.experimental.pallas import tpu as pltpu
from jax.sharding import PartitionSpec as P

MESH = pl.DeviceIdType.MESH
FW = 32
REACH = 2
COIL_DEV = 8
SPOKE_DEV = 32
X_DEV = 4
Z_DEV = 8
SLOTS = 8
Z_ORDER = (0, 1, 7, 2, 6, 3, 5, 4)
ROWS = 8
BLOCK = ROWS + 2 * REACH
PAIRS = BLOCK // 2
EARLY = SLOTS * (BLOCK - 2)
COLS = 128
GROUPS = 4
PER = SPOKE_DEV // GROUPS
BAND = 3 * 16 * PER
F32 = jnp.float32
BF16 = jnp.bfloat16


def kernel(distance):
    inner = jnp.maximum(1.0 - distance * distance * 0.25, 0.0)
    return inner * inner


def depth_table(length):
    phase = 2.0 * np.pi / length * (np.outer(np.arange(length), np.arange(length)) % length)
    c, s = np.cos(phase) / math.sqrt(length), np.sin(phase) / math.sqrt(length)
    return np.block([[c, -s], [s, c]])


def column_table(length):
    phase = 2.0 * np.pi / length * (np.outer(np.arange(length), np.arange(length)) % length)
    c, s = np.cos(phase) / math.sqrt(length), np.sin(phase) / math.sqrt(length)
    return np.block([[c, s], [-s, c]])


def in_two(exact):
    coarse = np.asarray(exact, BF16)
    return jnp.asarray(np.stack([coarse, np.asarray(exact - coarse.astype(np.float64), BF16)]))


def thirds(x):
    high = x.astype(BF16)
    rest = x - high.astype(F32)
    mid = rest.astype(BF16)
    low = (rest - mid.astype(F32)).astype(BF16)
    return high, mid, low


def dot_nt(a, b):
    return lax.dot_general(a, b, (((1,), (1,)), ((), ())), preferred_element_type=F32)


def dot(a, b):
    return jnp.dot(a, b, preferred_element_type=F32)


def body(
    live_ref, owner_hbm, table_hbm, coords_hbm, foot_hbm, index_hbm, kdata_hbm, depth_hbm, column_hbm,
    images, combined_ref,
    owner_ref, table_ref, coords_ref, foot_ref, index_ref, kd, depth_ref, column_ref, select, stage, send, recv, geo_send, geo, weights, fold, grid, power, power_send, power_recv,
    load_sem, geo_ssem, geo_rsem, pass_ssem, pass_rsem, val_ssem, val_rsem, pow_ssem, pow_rsem,
):
    me = lax.axis_index("spoke")
    coil = lax.axis_index("coil")
    x, z = me // Z_DEV, lax.rem(me, Z_DEV)
    x_at = [lax.rem(x + dx, X_DEV) * Z_DEV for dx in range(X_DEV)]
    z_at = [lax.rem(z + dz, Z_DEV) for dz in range(Z_DEV)]
    coil_at = [lax.rem(coil + step, COIL_DEV) for step in range(COIL_DEV)]

    def away(slot):
        return x_at[slot // Z_DEV] + z_at[Z_ORDER[slot % Z_DEV]]

    barrier = pltpu.get_barrier_semaphore()
    for slot in reversed(range(1, SPOKE_DEV)):
        pl.semaphore_signal(barrier, inc=1, device_id=(coil, away(slot)), device_id_type=MESH)
    for step in range(1, COIL_DEV):
        pl.semaphore_signal(barrier, inc=1, device_id=(coil_at[step], me), device_id_type=MESH)

    held = (owner_ref, table_ref, coords_ref, foot_ref, index_ref, kd, depth_ref, column_ref)
    given = (owner_hbm, table_hbm, coords_hbm, foot_hbm, index_hbm, kdata_hbm, depth_hbm, column_hbm)
    loads = [pltpu.make_async_copy(a, b, load_sem.at[i]) for i, (a, b) in enumerate(zip(given, held))]
    for load in loads:
        load.start()

    for load in loads[:5]:
        load.wait()
    row_of = lax.broadcasted_iota(jnp.int32, (8, 256), 0)
    entry = index_ref[...]
    density = jnp.zeros((8, 256), F32)
    for n in range(table_ref.shape[0]):
        density = jnp.where(entry == n, table_ref[n], density)
    density = jnp.where(row_of < live_ref[0], density, 0.0)
    foot = jnp.concatenate([foot_ref[...].astype(F32), jnp.zeros((8, 256 - SPOKE_DEV), F32)], axis=1)
    parts = []
    for comp in (coords_ref[:, 0, :], coords_ref[:, 1, :], density, foot):
        parts.extend(t.astype(F32) for t in thirds(comp))
    geometry = jnp.concatenate(parts, axis=0).astype(BF16)
    sample = lax.broadcasted_iota(jnp.int32, (256, 128), 0)
    lane = lax.broadcasted_iota(jnp.int32, (256, 128), 1)
    offset = lax.rem(lane, 32)
    group_of = lax.broadcasted_iota(jnp.int32, (8, 128), 1) // 32
    half, odd = (coil + 1) // 2, lax.rem(coil, 2)
    z_geo = lax.rem(z + odd * half + (1 - odd) * (Z_DEV - half), Z_DEV)
    for t in range(GROUPS):
        slab = owner_ref[x_at[t] + z_geo]
        near = (lane < 96) & (offset < BLOCK) & (sample == slab * ROWS - REACH + offset)
        hit = jnp.where(near | ((lane >= 96) & (sample == slab)), 1.0, 0.0).astype(BF16)
        got = dot(geometry, hit)
        tile = jnp.zeros((8, 128), F32)
        for c in range(4):
            part = got[24 * c : 24 * c + 8] + got[24 * c + 8 : 24 * c + 16] + got[24 * c + 16 : 24 * c + 24]
            tile = jnp.where(group_of == c, part, tile)
        geo_send[t] = tile

    row = lax.broadcasted_iota(jnp.int32, (4 * BLOCK, 256), 0)
    column = lax.broadcasted_iota(jnp.int32, (4 * BLOCK, 256), 1)
    for b in range(SPOKE_DEV // 4):
        wanted = owner_ref[4 * b] * ROWS - REACH + row
        for k in range(1, 4):
            wanted = jnp.where(row >= k * BLOCK, owner_ref[4 * b + k] * ROWS - REACH - k * BLOCK + row, wanted)
        select[b * 4 * BLOCK : (b + 1) * 4 * BLOCK, :] = jnp.where(wanted == column, 1.0, 0.0).astype(BF16)

    def fill(c):
        for p in range(SLOTS):
            stage[pl.ds(p, SPOKE_DEV * BLOCK, stride=SLOTS), :] = dot_nt(
                select[...], kd[p, c * COLS : (c + 1) * COLS, :]
            )
        send[:, :, c * COLS : (c + 1) * COLS] = stage[...].astype(BF16).reshape(SPOKE_DEV, BLOCK * SLOTS, COLS)

    loads[5].wait()
    fill(0)
    fill(1)

    pl.semaphore_wait(barrier, SPOKE_DEV - 1 + COIL_DEV - 1)

    def geo_copy(t):
        return pltpu.make_async_remote_copy(
            geo_send.at[t],
            geo.at[coil, t],
            geo_ssem.at[t],
            geo_rsem.at[t],
            device_id=(coil, x_at[t] + z_geo),
            device_id_type=MESH,
        )

    def value_copy(c, slot, dest):
        rows = (pl.ds(0, EARLY), pl.ds(EARLY, BLOCK * SLOTS - EARLY))[c]
        return pltpu.make_async_remote_copy(
            send.at[dest, rows],
            recv.at[slot, rows],
            val_ssem.at[c, slot],
            val_rsem.at[c, slot],
            device_id=(coil, dest),
            device_id_type=MESH,
        )

    def pass_copy(step):
        return pltpu.make_async_remote_copy(
            geo.at[coil],
            geo.at[coil],
            pass_ssem.at[step],
            pass_rsem.at[step],
            device_id=(lax.rem(coil + step, COIL_DEV), me),
            device_id_type=MESH,
        )

    def pass_arrival(step):
        source = lax.rem(coil - step + COIL_DEV, COIL_DEV)
        return pltpu.make_async_remote_copy(
            geo.at[source],
            geo.at[source],
            pass_ssem.at[step],
            pass_rsem.at[step],
            device_id=(lax.rem(coil + step, COIL_DEV), me),
            device_id_type=MESH,
        )

    for t in range(1, GROUPS):
        geo_copy(t).start()

    @pl.when(coil != 0)
    def _():
        geo_copy(0).start()

    @pl.when(coil == 0)
    def _():
        geo[0, 0] = geo_send[0]

    for c in range(2):
        for slot in range(1, SPOKE_DEV):
            value_copy(c, slot, away(slot)).start()

    recv[0] = send[me]

    for t in range(1, GROUPS):
        geo_copy(t).wait_recv()

    @pl.when(coil != 0)
    def _():
        geo_copy(0).wait_recv()

    @pl.loop(1, COIL_DEV)
    def _(step):
        pass_copy(step).start()

    @pl.loop(1, COIL_DEV)
    def _(step):
        pass_arrival(step).wait_recv()

    first_row = (owner_ref[me] * ROWS).astype(F32)
    cells = lax.broadcasted_iota(jnp.int32, (8, 256), 1).astype(F32)

    @pl.loop(0, SPOKE_DEV)
    def _(slot):
        group = slot // PER
        member = lax.rem(slot, PER)
        tile = geo[lax.rem(slot, 8), slot // 8]

        def spread(comp, j):
            lane = comp * 32 + j
            return jnp.broadcast_to(tile[:, lane : lane + 1], (8, 256))

        across, along = [], []
        for j in range(BLOCK):
            start = spread(3, j)
            covered = (cells >= start) & (cells < start + FW)
            across.append(jnp.where(covered, kernel(cells + 0.5 - spread(1, j)), 0.0))
            along.append((spread(0, j)[:, :128], spread(2, j)[:, :128]))
        at = pl.multiple_of(member * 16, 16)
        for g in range(ROWS):
            for i in range(3):
                pair = []
                for j in (2 * (g // 2 + i), 2 * (g // 2 + i) + 1):
                    row, dens = along[j]
                    value = dens * kernel(first_row + (g + 0.5) - row)
                    pair.append(jnp.concatenate([value, value], axis=1) * across[j])
                weights[group, g, pl.ds(i * 16 * PER + at, 16), :] = jnp.concatenate(pair, axis=0).astype(BF16)

    for load in loads[6:]:
        load.wait()

    def arrived(c, q):
        @pl.loop(max(1, q * PER), (q + 1) * PER)
        def _(slot):
            value_copy(c, slot, x_at[1]).wait_recv()

    def folded(i, q, c):
        got = recv[q * PER : (q + 1) * PER, i * 16 : (i + 1) * 16, c * COLS : (c + 1) * COLS].reshape(16 * PER, COLS)
        both = dot_nt(depth_ref[0], got) + dot_nt(depth_ref[1], got)
        fold[:, i * 16 * PER : (i + 1) * 16 * PER] = both.astype(BF16)

    def transform(c, h):
        spectrum = jnp.concatenate(
            [jnp.concatenate([grid[c, g, :64], grid[c, g, 64:]], axis=1) for g in (2 * h, 2 * h + 1)], axis=0
        ).astype(BF16)
        turned = dot(spectrum, column_ref[0]) + dot(spectrum, column_ref[1])
        for g in (2 * h, 2 * h + 1):
            at = (g - 2 * h) * 64
            real, imag = turned[at : at + 64, :256], turned[at : at + 64, 256:]
            images[g, c, 0] = real
            images[g, c, 1] = imag
            mine = real * real + imag * imag
            power[g] = mine if c == 0 else power[g] + mine

    def share(h):
        for k in range(COIL_DEV):
            power_send[h, k] = jnp.concatenate(
                [power[g, 8 * k : 8 * k + 8] for g in (2 * h, 2 * h + 1)], axis=0
            ).astype(BF16)
        for step in range(1, COIL_DEV):
            power_copy(h, step).start()

    def power_copy(h, step):
        return pltpu.make_async_remote_copy(
            power_send.at[h, coil_at[step]],
            power_recv.at[h, step],
            pow_ssem.at[h, step],
            pow_rsem.at[h, step],
            device_id=(coil_at[step], me),
            device_id_type=MESH,
        )

    last = PAIRS - 1
    for q in range(GROUPS):
        arrived(0, q)
        for c in range(2):
            for i in range(last):
                folded(i, q, c)
            for g in range(ROWS):
                depth = BAND if g // 2 + 2 < last else BAND - 16 * PER
                at = (g // 2) * 16 * PER
                term = dot(fold[:, at : at + depth], weights[q, g, :depth])
                grid[c, g] = term if q == 0 else grid[c, g] + term
    for h in range(ROWS // 2 - 1):
        transform(0, h)
        transform(1, h)
        share(h)
    for q in range(GROUPS):
        arrived(1, q)
        for c in range(2):
            folded(last, q, c)
            got = fold[:, last * 16 * PER :]
            for g in (ROWS - 2, ROWS - 1):
                grid[c, g] = grid[c, g] + dot(got, weights[q, g, BAND - 16 * PER :])
    for c in range(2):
        transform(c, ROWS // 2 - 1)
    share(ROWS // 2 - 1)

    for h in range(ROWS // 2):
        power_recv[h, 0] = power_send[h, coil]
        for step in range(1, COIL_DEV):
            power_copy(h, step).wait_recv()
        total = power_recv[h, 0].astype(F32)
        for k in range(1, COIL_DEV):
            total = total + power_recv[h, k].astype(F32)
        combined = jnp.sqrt(total)
        combined_ref[2 * h] = combined[:8]
        combined_ref[2 * h + 1] = combined[8:]

    for c in range(2):

        @pl.loop(1, SPOKE_DEV)
        def _(slot):
            value_copy(c, slot, x_at[1]).wait_send()

    for t in range(1, GROUPS):
        geo_copy(t).wait_send()

    @pl.when(coil != 0)
    def _():
        geo_copy(0).wait_send()

    @pl.loop(1, COIL_DEV)
    def _(step):
        pass_copy(step).wait_send()

    for h in range(ROWS // 2):
        for step in range(1, COIL_DEV):
            power_copy(h, step).wait_send()


def written(images, combined, images_out, combined_out, sem):
    copies = [
        pltpu.make_async_copy(images, images_out, sem.at[0]),
        pltpu.make_async_copy(combined, combined_out, sem.at[1]),
    ]
    for copy in copies:
        copy.start()
    for copy in copies:
        copy.wait()


def on_device(kdata, coords, foot_offset, live_count, dcf_table, dcf_index, slab_owner):
    slots, coil_dev, parts, kz, samp = kdata.shape
    kd = kdata.reshape(slots, coil_dev * parts * kz, samp)
    depth = in_two(depth_table(kz))
    column = in_two(column_table(samp))
    vmem = pl.BlockSpec(memory_space=pltpu.VMEM)
    hbm = pl.BlockSpec(memory_space=pltpu.HBM)
    dma = pltpu.SemaphoreType.DMA
    images, combined = pl.pallas_call(
        body,
        out_shape=(
            jax.ShapeDtypeStruct((ROWS, coil_dev, parts, kz, samp), F32),
            jax.ShapeDtypeStruct((ROWS, kz // COIL_DEV, samp), F32),
        ),
        in_specs=[pl.BlockSpec(memory_space=pltpu.SMEM)] + [hbm] * 8,
        out_specs=(vmem, vmem),
        scratch_shapes=[
            pltpu.SMEM(slab_owner.shape, jnp.int32),
            pltpu.SMEM(dcf_table.shape, F32),
            pltpu.VMEM(coords.shape, F32),
            pltpu.VMEM(foot_offset.shape, jnp.int32),
            pltpu.VMEM(dcf_index.shape, jnp.int32),
            pltpu.VMEM(kd.shape, BF16),
            pltpu.VMEM(depth.shape, BF16),
            pltpu.VMEM(column.shape, BF16),
            pltpu.VMEM((SPOKE_DEV * BLOCK, samp), BF16),
            pltpu.VMEM((SPOKE_DEV * BLOCK * SLOTS, COLS), F32),
            pltpu.VMEM((SPOKE_DEV, BLOCK * SLOTS, 2 * COLS), BF16),
            pltpu.VMEM((SPOKE_DEV, BLOCK * SLOTS, 2 * COLS), BF16),
            pltpu.VMEM((GROUPS, 8, 128), F32),
            pltpu.VMEM((COIL_DEV, GROUPS, 8, 128), F32),
            pltpu.VMEM((GROUPS, ROWS, BAND, 256), BF16),
            pltpu.VMEM((COLS, PAIRS * 16 * PER), BF16),
            pltpu.VMEM((2, ROWS, COLS, 256), F32),
            pltpu.VMEM((ROWS, kz, samp), F32),
            pltpu.VMEM((ROWS // 2, COIL_DEV, 16, samp), BF16),
            pltpu.VMEM((ROWS // 2, COIL_DEV, 16, samp), BF16),
            dma((8,)),
            dma((GROUPS,)),
            dma((GROUPS,)),
            dma((COIL_DEV,)),
            dma((COIL_DEV,)),
            dma((2, SPOKE_DEV)),
            dma((2, SPOKE_DEV)),
            dma((ROWS // 2, COIL_DEV)),
            dma((ROWS // 2, COIL_DEV)),
        ],
        compiler_params=pltpu.CompilerParams(
            collective_id=0, has_side_effects=True, vmem_limit_bytes=24 * 2**20
        ),
    )(
        live_count,
        *(
            pltpu.with_memory_space_constraint(a, pltpu.HBM)
            for a in (slab_owner, dcf_table, coords, foot_offset, dcf_index, kd, depth, column)
        ),
    )
    return pl.pallas_call(
        written,
        out_shape=(
            jax.ShapeDtypeStruct(images.shape, F32),
            jax.ShapeDtypeStruct(combined.shape, F32),
        ),
        in_specs=[hbm] * 2,
        out_specs=(hbm, hbm),
        scratch_shapes=[dma((2,))],
        compiler_params=pltpu.CompilerParams(vmem_limit_bytes=2**20),
    )(images, combined)


def solution(mesh):
    return jax.shard_map(
        on_device,
        mesh=mesh,
        in_specs=(
            P("spoke", "coil", None, None, None),
            P("spoke", None, None),
            P("spoke", None),
            P("spoke"),
            P(),
            P("spoke", None),
            P(),
        ),
        out_specs=(P("spoke", "coil", None, None, None), P("spoke", "coil", None)),
        check_vma=False,
    )
```

```python
import math

import jax
import jax.numpy as jnp
import numpy as np
from jax import lax
from jax.experimental import pallas as pl
from jax.experimental.pallas import tpu as pltpu
from jax.sharding import PartitionSpec as P

MESH = pl.DeviceIdType.MESH
FW = 32
REACH = 2
COIL_DEV = 8
SPOKE_DEV = 32
X_DEV = 4
Z_DEV = 8
SLOTS = 8
Z_ORDER = (0, 1, 7, 2, 6, 3, 5, 4)
ROWS = 8
BLOCK = ROWS + 2 * REACH
PAIRS = BLOCK // 2
EARLY = SLOTS * (BLOCK - 2)
COLS = 128
GROUPS = 4
CARRY = 4
TILES = SPOKE_DEV // CARRY
POWER_PARTS = ((0, 1, 2), (3,))
PER = SPOKE_DEV // GROUPS
BAND = 3 * 16 * PER
F32 = jnp.float32
BF16 = jnp.bfloat16


def kernel(distance):
    inner = jnp.maximum(1.0 - distance * distance * 0.25, 0.0)
    return inner * inner


def depth_table(length):
    phase = 2.0 * np.pi / length * (np.outer(np.arange(length), np.arange(length)) % length)
    c, s = np.cos(phase) / math.sqrt(length), np.sin(phase) / math.sqrt(length)
    return np.block([[c, -s], [s, c]])


def column_table(length):
    phase = 2.0 * np.pi / length * (np.outer(np.arange(length), np.arange(length)) % length)
    c, s = np.cos(phase) / math.sqrt(length), np.sin(phase) / math.sqrt(length)
    return np.block([[c, s], [-s, c]])


def in_two(exact):
    coarse = np.asarray(exact, BF16)
    return jnp.asarray(np.stack([coarse, np.asarray(exact - coarse.astype(np.float64), BF16)]))


def thirds(x):
    high = x.astype(BF16)
    rest = x - high.astype(F32)
    mid = rest.astype(BF16)
    low = (rest - mid.astype(F32)).astype(BF16)
    return high, mid, low


def dot_nt(a, b):
    return lax.dot_general(a, b, (((1,), (1,)), ((), ())), preferred_element_type=F32)


def dot(a, b):
    return jnp.dot(a, b, preferred_element_type=F32)


def body(
    live_ref, owner_hbm, table_hbm, coords_hbm, foot_hbm, index_hbm, kdata_hbm, depth_hbm, column_hbm,
    images, combined_ref,
    owner_ref, table_ref, coords_ref, foot_ref, index_ref, kd, depth_ref, column_ref, select, stage, send, recv, geo_send, geo, weights, fold, grid, power, power_send, power_recv,
    load_sem, geo_ssem, geo_rsem, pass_ssem, pass_rsem, val_ssem, val_rsem, pow_ssem, pow_rsem,
):
    me = lax.axis_index("spoke")
    coil = lax.axis_index("coil")
    x, z = me // Z_DEV, lax.rem(me, Z_DEV)
    x_at = [lax.rem(x + dx, X_DEV) * Z_DEV for dx in range(X_DEV)]
    z_at = [lax.rem(z + dz, Z_DEV) for dz in range(Z_DEV)]
    coil_at = [lax.rem(coil + step, COIL_DEV) for step in range(COIL_DEV)]

    def away(slot):
        return x_at[slot // Z_DEV] + z_at[Z_ORDER[slot % Z_DEV]]

    barrier = pltpu.get_barrier_semaphore()
    for slot in reversed(range(1, SPOKE_DEV)):
        pl.semaphore_signal(barrier, inc=1, device_id=(coil, away(slot)), device_id_type=MESH)
    for step in range(1, COIL_DEV):
        pl.semaphore_signal(barrier, inc=1, device_id=(coil_at[step], me), device_id_type=MESH)

    held = (owner_ref, table_ref, coords_ref, foot_ref, index_ref, kd, depth_ref, column_ref)
    given = (owner_hbm, table_hbm, coords_hbm, foot_hbm, index_hbm, kdata_hbm, depth_hbm, column_hbm)
    loads = [pltpu.make_async_copy(a, b, load_sem.at[i]) for i, (a, b) in enumerate(zip(given, held))]
    for load in loads:
        load.start()

    for load in loads[:5]:
        load.wait()
    row_of = lax.broadcasted_iota(jnp.int32, (8, 256), 0)
    entry = index_ref[...]
    density = jnp.zeros((8, 256), F32)
    for n in range(table_ref.shape[0]):
        density = jnp.where(entry == n, table_ref[n], density)
    density = jnp.where(row_of < live_ref[0], density, 0.0)
    foot = jnp.concatenate([foot_ref[...].astype(F32), jnp.zeros((8, 256 - SPOKE_DEV), F32)], axis=1)
    parts = []
    for comp in (coords_ref[:, 0, :], coords_ref[:, 1, :], density, foot):
        parts.extend(t.astype(F32) for t in thirds(comp))
    geometry = jnp.concatenate(parts, axis=0).astype(BF16)
    sample = lax.broadcasted_iota(jnp.int32, (256, 128), 0)
    lane = lax.broadcasted_iota(jnp.int32, (256, 128), 1)
    offset = lax.rem(lane, 32)
    group_of = lax.broadcasted_iota(jnp.int32, (8, 128), 1) // 32
    z_geo = []
    for k in range(2):
        r = coil + k * CARRY
        odd = lax.rem(r, 2)
        dz = odd * ((r + 1) // 2) + (1 - odd) * (Z_DEV - r // 2)
        z_geo.append(lax.rem(z + dz, Z_DEV))

    def geo_dest(t):
        return x_at[t // 2] + z_geo[t % 2]

    @pl.when(coil < CARRY)
    def _():
        for t in range(TILES):
            slab = owner_ref[geo_dest(t)]
            near = (lane < 96) & (offset < BLOCK) & (sample == slab * ROWS - REACH + offset)
            hit = jnp.where(near | ((lane >= 96) & (sample == slab)), 1.0, 0.0).astype(BF16)
            got = dot(geometry, hit)
            tile = jnp.zeros((8, 128), F32)
            for c in range(4):
                part = got[24 * c : 24 * c + 8] + got[24 * c + 8 : 24 * c + 16] + got[24 * c + 16 : 24 * c + 24]
                tile = jnp.where(group_of == c, part, tile)
            geo_send[t] = tile

    row = lax.broadcasted_iota(jnp.int32, (4 * BLOCK, 256), 0)
    column = lax.broadcasted_iota(jnp.int32, (4 * BLOCK, 256), 1)
    for b in range(SPOKE_DEV // 4):
        wanted = owner_ref[4 * b] * ROWS - REACH + row
        for k in range(1, 4):
            wanted = jnp.where(row >= k * BLOCK, owner_ref[4 * b + k] * ROWS - REACH - k * BLOCK + row, wanted)
        select[b * 4 * BLOCK : (b + 1) * 4 * BLOCK, :] = jnp.where(wanted == column, 1.0, 0.0).astype(BF16)

    def fill(c):
        for p in range(SLOTS):
            stage[pl.ds(p, SPOKE_DEV * BLOCK, stride=SLOTS), :] = dot_nt(
                select[...], kd[p, c * COLS : (c + 1) * COLS, :]
            )
        send[:, :, c * COLS : (c + 1) * COLS] = stage[...].astype(BF16).reshape(SPOKE_DEV, BLOCK * SLOTS, COLS)

    loads[5].wait()
    fill(0)
    fill(1)

    pl.semaphore_wait(barrier, SPOKE_DEV - 1 + COIL_DEV - 1)

    def geo_copy(t):
        return pltpu.make_async_remote_copy(
            geo_send.at[t],
            geo.at[coil, t],
            geo_ssem.at[t],
            geo_rsem.at[t],
            device_id=(coil, geo_dest(t)),
            device_id_type=MESH,
        )

    def value_copy(c, slot, dest):
        rows = (pl.ds(0, EARLY), pl.ds(EARLY, BLOCK * SLOTS - EARLY))[c]
        return pltpu.make_async_remote_copy(
            send.at[dest, rows],
            recv.at[slot, rows],
            val_ssem.at[c, slot],
            val_rsem.at[c, slot],
            device_id=(coil, dest),
            device_id_type=MESH,
        )

    def pass_copy(step):
        return pltpu.make_async_remote_copy(
            geo.at[coil],
            geo.at[coil],
            pass_ssem.at[step],
            pass_rsem.at[step],
            device_id=(lax.rem(coil + step, COIL_DEV), me),
            device_id_type=MESH,
        )

    def pass_arrival(source):
        step = lax.rem(coil - source + COIL_DEV, COIL_DEV)
        return pltpu.make_async_remote_copy(
            geo.at[source],
            geo.at[source],
            pass_ssem.at[step],
            pass_rsem.at[step],
            device_id=(coil_at[1], me),
            device_id_type=MESH,
        )

    @pl.when(coil < CARRY)
    def _():
        for t in range(1, TILES):
            geo_copy(t).start()

    @pl.when((coil > 0) & (coil < CARRY))
    def _():
        geo_copy(0).start()

    @pl.when(coil == 0)
    def _():
        geo[0, 0] = geo_send[0]

    for slot in range(1, SPOKE_DEV):
        value_copy(0, slot, away(slot)).start()
    for zt in (0, 1, 2, 3, 7, 4, 6, 5):
        dz = lax.rem(zt - z + Z_DEV, Z_DEV)
        back = (dz + 3) // 8
        ahead = (dz + 7) // 8 - back
        r = ahead * (2 * dz - 1) + back * (2 * (Z_DEV - dz))
        for dx in (0, 1, 3, 2):
            dest = x_at[dx] + zt

            @pl.when(dest != me)
            def _():
                value_copy(1, dx * Z_DEV + r, dest).start()


    recv[0] = send[me]

    @pl.when(coil < CARRY)
    def _():
        for t in range(1, TILES):
            geo_copy(t).wait_recv()

    @pl.when((coil > 0) & (coil < CARRY))
    def _():
        geo_copy(0).wait_recv()

    @pl.when(coil < CARRY)
    def _():
        for step in range(1, COIL_DEV):
            pass_copy(step).start()

    for source in range(CARRY):

        @pl.when(coil != source)
        def _():
            pass_arrival(source).wait_recv()

    first_row = (owner_ref[me] * ROWS).astype(F32)
    cells = lax.broadcasted_iota(jnp.int32, (8, 256), 1).astype(F32)

    @pl.loop(0, SPOKE_DEV)
    def _(slot):
        group = slot // PER
        member = lax.rem(slot, PER)
        tile = geo[lax.rem(slot, CARRY), slot // CARRY]

        def spread(comp, j):
            lane = comp * 32 + j
            return jnp.broadcast_to(tile[:, lane : lane + 1], (8, 256))

        across, along = [], []
        for j in range(BLOCK):
            start = spread(3, j)
            covered = (cells >= start) & (cells < start + FW)
            across.append(jnp.where(covered, kernel(cells + 0.5 - spread(1, j)), 0.0))
            along.append((spread(0, j)[:, :128], spread(2, j)[:, :128]))
        at = pl.multiple_of(member * 16, 16)
        for g in range(ROWS):
            for i in range(3):
                pair = []
                for j in (2 * (g // 2 + i), 2 * (g // 2 + i) + 1):
                    row, dens = along[j]
                    value = dens * kernel(first_row + (g + 0.5) - row)
                    pair.append(jnp.concatenate([value, value], axis=1) * across[j])
                weights[group, g, pl.ds(i * 16 * PER + at, 16), :] = jnp.concatenate(pair, axis=0).astype(BF16)

    for load in loads[6:]:
        load.wait()

    def arrived(c, q):
        @pl.loop(max(1, q * PER), (q + 1) * PER)
        def _(slot):
            value_copy(c, slot, x_at[1]).wait_recv()

    def folded(i, q, c):
        got = recv[q * PER : (q + 1) * PER, i * 16 : (i + 1) * 16, c * COLS : (c + 1) * COLS].reshape(16 * PER, COLS)
        both = dot_nt(depth_ref[0], got) + dot_nt(depth_ref[1], got)
        fold[:, i * 16 * PER : (i + 1) * 16 * PER] = both.astype(BF16)

    def transform(c, h):
        spectrum = jnp.concatenate(
            [jnp.concatenate([grid[c, g, :64], grid[c, g, 64:]], axis=1) for g in (2 * h, 2 * h + 1)], axis=0
        ).astype(BF16)
        turned = dot(spectrum, column_ref[0]) + dot(spectrum, column_ref[1])
        for g in (2 * h, 2 * h + 1):
            at = (g - 2 * h) * 64
            real, imag = turned[at : at + 64, :256], turned[at : at + 64, 256:]
            images[g, c, 0] = real
            images[g, c, 1] = imag
            mine = real * real + imag * imag
            power[g] = mine if c == 0 else power[g] + mine

    def share(part):
        for h in POWER_PARTS[part]:
            for k in range(COIL_DEV):
                power_send[k, 16 * h : 16 * h + 16] = jnp.concatenate(
                    [power[g, 8 * k : 8 * k + 8] for g in (2 * h, 2 * h + 1)], axis=0
                ).astype(BF16)
        for step in range(1, COIL_DEV):
            power_copy(part, step).start()

    def power_copy(part, step):
        rows = pl.ds(16 * POWER_PARTS[part][0], 16 * len(POWER_PARTS[part]))
        return pltpu.make_async_remote_copy(
            power_send.at[coil_at[step], rows],
            power_recv.at[step, rows],
            pow_ssem.at[part, step],
            pow_rsem.at[part, step],
            device_id=(coil_at[step], me),
            device_id_type=MESH,
        )

    last = PAIRS - 1
    for q in range(GROUPS):
        arrived(0, q)
        for c in range(2):
            for i in range(last):
                folded(i, q, c)
            for g in range(ROWS):
                depth = BAND if g // 2 + 2 < last else BAND - 16 * PER
                at = (g // 2) * 16 * PER
                term = dot(fold[:, at : at + depth], weights[q, g, :depth])
                grid[c, g] = term if q == 0 else grid[c, g] + term
    for h in range(ROWS // 2 - 1):
        transform(0, h)
        transform(1, h)
    share(0)
    for q in range(GROUPS):
        arrived(1, q)
        for c in range(2):
            folded(last, q, c)
            got = fold[:, last * 16 * PER :]
            for g in (ROWS - 2, ROWS - 1):
                grid[c, g] = grid[c, g] + dot(got, weights[q, g, BAND - 16 * PER :])
    for c in range(2):
        transform(c, ROWS // 2 - 1)
    share(1)

    for part, lines in enumerate(POWER_PARTS):
        for step in range(1, COIL_DEV):
            power_copy(part, step).wait_recv()
        for h in lines:
            rows = pl.ds(16 * h, 16)
            total = power_send[coil, rows].astype(F32)
            for k in range(1, COIL_DEV):
                total = total + power_recv[k, rows].astype(F32)
            combined = jnp.sqrt(total)
            combined_ref[2 * h] = combined[:8]
            combined_ref[2 * h + 1] = combined[8:]

    for c in range(2):

        @pl.loop(1, SPOKE_DEV)
        def _(slot):
            value_copy(c, slot, x_at[1]).wait_send()

    @pl.when(coil < CARRY)
    def _():
        for t in range(1, TILES):
            geo_copy(t).wait_send()
        for step in range(1, COIL_DEV):
            pass_copy(step).wait_send()

    @pl.when((coil > 0) & (coil < CARRY))
    def _():
        geo_copy(0).wait_send()

    for part in range(len(POWER_PARTS)):
        for step in range(1, COIL_DEV):
            power_copy(part, step).wait_send()


def written(images, combined, images_out, combined_out, sem):
    copies = [
        pltpu.make_async_copy(images, images_out, sem.at[0]),
        pltpu.make_async_copy(combined, combined_out, sem.at[1]),
    ]
    for copy in copies:
        copy.start()
    for copy in copies:
        copy.wait()


def on_device(kdata, coords, foot_offset, live_count, dcf_table, dcf_index, slab_owner):
    slots, coil_dev, parts, kz, samp = kdata.shape
    kd = kdata.reshape(slots, coil_dev * parts * kz, samp)
    depth = in_two(depth_table(kz))
    column = in_two(column_table(samp))
    vmem = pl.BlockSpec(memory_space=pltpu.VMEM)
    hbm = pl.BlockSpec(memory_space=pltpu.HBM)
    dma = pltpu.SemaphoreType.DMA
    images, combined = pl.pallas_call(
        body,
        out_shape=(
            jax.ShapeDtypeStruct((ROWS, coil_dev, parts, kz, samp), F32),
            jax.ShapeDtypeStruct((ROWS, kz // COIL_DEV, samp), F32),
        ),
        in_specs=[pl.BlockSpec(memory_space=pltpu.SMEM)] + [hbm] * 8,
        out_specs=(vmem, vmem),
        scratch_shapes=[
            pltpu.SMEM(slab_owner.shape, jnp.int32),
            pltpu.SMEM(dcf_table.shape, F32),
            pltpu.VMEM(coords.shape, F32),
            pltpu.VMEM(foot_offset.shape, jnp.int32),
            pltpu.VMEM(dcf_index.shape, jnp.int32),
            pltpu.VMEM(kd.shape, BF16),
            pltpu.VMEM(depth.shape, BF16),
            pltpu.VMEM(column.shape, BF16),
            pltpu.VMEM((SPOKE_DEV * BLOCK, samp), BF16),
            pltpu.VMEM((SPOKE_DEV * BLOCK * SLOTS, COLS), F32),
            pltpu.VMEM((SPOKE_DEV, BLOCK * SLOTS, 2 * COLS), BF16),
            pltpu.VMEM((SPOKE_DEV, BLOCK * SLOTS, 2 * COLS), BF16),
            pltpu.VMEM((TILES, 8, 128), F32),
            pltpu.VMEM((CARRY, TILES, 8, 128), F32),
            pltpu.VMEM((GROUPS, ROWS, BAND, 256), BF16),
            pltpu.VMEM((COLS, PAIRS * 16 * PER), BF16),
            pltpu.VMEM((2, ROWS, COLS, 256), F32),
            pltpu.VMEM((ROWS, kz, samp), F32),
            pltpu.VMEM((COIL_DEV, ROWS * 8, samp), BF16),
            pltpu.VMEM((COIL_DEV, ROWS * 8, samp), BF16),
            dma((8,)),
            dma((TILES,)),
            dma((TILES,)),
            dma((COIL_DEV,)),
            dma((COIL_DEV,)),
            dma((2, SPOKE_DEV)),
            dma((2, SPOKE_DEV)),
            dma((len(POWER_PARTS), COIL_DEV)),
            dma((len(POWER_PARTS), COIL_DEV)),
        ],
        compiler_params=pltpu.CompilerParams(
            collective_id=0, has_side_effects=True, vmem_limit_bytes=24 * 2**20
        ),
    )(
        live_count,
        *(
            pltpu.with_memory_space_constraint(a, pltpu.HBM)
            for a in (slab_owner, dcf_table, coords, foot_offset, dcf_index, kd, depth, column)
        ),
    )
    return pl.pallas_call(
        written,
        out_shape=(
            jax.ShapeDtypeStruct(images.shape, F32),
            jax.ShapeDtypeStruct(combined.shape, F32),
        ),
        in_specs=[hbm] * 2,
        out_specs=(hbm, hbm),
        scratch_shapes=[dma((2,))],
        compiler_params=pltpu.CompilerParams(vmem_limit_bytes=2**20),
    )(images, combined)


def solution(mesh):
    return jax.shard_map(
        on_device,
        mesh=mesh,
        in_specs=(
            P("spoke", "coil", None, None, None),
            P("spoke", None, None),
            P("spoke", None),
            P("spoke"),
            P(),
            P("spoke", None),
            P(),
        ),
        out_specs=(P("spoke", "coil", None, None, None), P("spoke", "coil", None)),
        check_vma=False,
    )
```

```python
import math

import jax
import jax.numpy as jnp
import numpy as np
from jax import lax
from jax.experimental import pallas as pl
from jax.experimental.pallas import tpu as pltpu
from jax.sharding import PartitionSpec as P

MESH = pl.DeviceIdType.MESH
FW = 32
REACH = 2
COIL_DEV = 8
SPOKE_DEV = 32
X_DEV = 4
Z_DEV = 8
SLOTS = 8
Z_ORDER = (0, 1, 7, 2, 6, 3, 5, 4)
ROWS = 8
BLOCK = ROWS + 2 * REACH
PAIRS = BLOCK // 2
EARLY = SLOTS * (BLOCK - 2)
COLS = 128
GROUPS = 4
CARRY = 4
TILES = SPOKE_DEV // CARRY
POWER_PARTS = ((0, 1, 2), (3,))
PER = SPOKE_DEV // GROUPS
BAND = 3 * 16 * PER
F32 = jnp.float32
BF16 = jnp.bfloat16


def kernel(distance):
    inner = jnp.maximum(1.0 - distance * distance * 0.25, 0.0)
    return inner * inner


def depth_table(length):
    phase = 2.0 * np.pi / length * (np.outer(np.arange(length), np.arange(length)) % length)
    c, s = np.cos(phase) / math.sqrt(length), np.sin(phase) / math.sqrt(length)
    return np.block([[c, -s], [s, c]])


def column_table(length):
    phase = 2.0 * np.pi / length * (np.outer(np.arange(length), np.arange(length)) % length)
    c, s = np.cos(phase) / math.sqrt(length), np.sin(phase) / math.sqrt(length)
    return np.block([[c, s], [-s, c]])


def in_two(exact):
    coarse = np.asarray(exact, BF16)
    return jnp.asarray(np.stack([coarse, np.asarray(exact - coarse.astype(np.float64), BF16)]))


def thirds(x):
    high = x.astype(BF16)
    rest = x - high.astype(F32)
    mid = rest.astype(BF16)
    low = (rest - mid.astype(F32)).astype(BF16)
    return high, mid, low


def dot_nt(a, b):
    return lax.dot_general(a, b, (((1,), (1,)), ((), ())), preferred_element_type=F32)


def dot(a, b):
    return jnp.dot(a, b, preferred_element_type=F32)


def body(
    live_ref, owner_hbm, table_hbm, coords_hbm, foot_hbm, index_hbm, kdata_hbm, depth_hbm, column_hbm,
    images, combined_ref,
    owner_ref, table_ref, coords_ref, foot_ref, index_ref, kd, depth_ref, column_ref, select, stage, send, recv, geo_send, geo, weights, fold, grid, power, power_send, power_recv,
    load_sem, geo_ssem, geo_rsem, pass_ssem, pass_rsem, val_ssem, val_rsem, pow_ssem, pow_rsem,
):
    me = lax.axis_index("spoke")
    coil = lax.axis_index("coil")
    x, z = me // Z_DEV, lax.rem(me, Z_DEV)
    x_at = [lax.rem(x + dx, X_DEV) * Z_DEV for dx in range(X_DEV)]
    z_at = [lax.rem(z + dz, Z_DEV) for dz in range(Z_DEV)]
    coil_at = [lax.rem(coil + step, COIL_DEV) for step in range(COIL_DEV)]

    def away(slot):
        return x_at[slot // Z_DEV] + z_at[Z_ORDER[slot % Z_DEV]]

    barrier = pltpu.get_barrier_semaphore()
    for slot in reversed(range(1, SPOKE_DEV)):
        pl.semaphore_signal(barrier, inc=1, device_id=(coil, away(slot)), device_id_type=MESH)
    for step in range(1, COIL_DEV):
        pl.semaphore_signal(barrier, inc=1, device_id=(coil_at[step], me), device_id_type=MESH)

    held = (owner_ref, table_ref, coords_ref, foot_ref, index_ref, kd, depth_ref, column_ref)
    given = (owner_hbm, table_hbm, coords_hbm, foot_hbm, index_hbm, kdata_hbm, depth_hbm, column_hbm)
    loads = [pltpu.make_async_copy(a, b, load_sem.at[i]) for i, (a, b) in enumerate(zip(given, held))]
    for load in loads:
        load.start()

    for load in loads[:5]:
        load.wait()
    row_of = lax.broadcasted_iota(jnp.int32, (8, 256), 0)
    entry = index_ref[...]
    density = jnp.zeros((8, 256), F32)
    for n in range(table_ref.shape[0]):
        density = jnp.where(entry == n, table_ref[n], density)
    density = jnp.where(row_of < live_ref[0], density, 0.0)
    foot = jnp.concatenate([foot_ref[...].astype(F32), jnp.zeros((8, 256 - SPOKE_DEV), F32)], axis=1)
    parts = []
    for comp in (coords_ref[:, 0, :], coords_ref[:, 1, :], density, foot):
        parts.extend(t.astype(F32) for t in thirds(comp))
    geometry = jnp.concatenate(parts, axis=0).astype(BF16)
    sample = lax.broadcasted_iota(jnp.int32, (256, 128), 0)
    lane = lax.broadcasted_iota(jnp.int32, (256, 128), 1)
    offset = lax.rem(lane, 32)
    group_of = lax.broadcasted_iota(jnp.int32, (8, 128), 1) // 32
    z_geo = []
    for k in range(2):
        r = coil + k * CARRY
        odd = lax.rem(r, 2)
        dz = odd * ((r + 1) // 2) + (1 - odd) * (Z_DEV - r // 2)
        z_geo.append(lax.rem(z + dz, Z_DEV))

    def geo_dest(t):
        return x_at[t // 2] + z_geo[t % 2]

    @pl.when(coil < CARRY)
    def _():
        for t in range(TILES):
            slab = owner_ref[geo_dest(t)]
            near = (lane < 96) & (offset < BLOCK) & (sample == slab * ROWS - REACH + offset)
            hit = jnp.where(near | ((lane >= 96) & (sample == slab)), 1.0, 0.0).astype(BF16)
            got = dot(geometry, hit)
            tile = jnp.zeros((8, 128), F32)
            for c in range(4):
                part = got[24 * c : 24 * c + 8] + got[24 * c + 8 : 24 * c + 16] + got[24 * c + 16 : 24 * c + 24]
                tile = jnp.where(group_of == c, part, tile)
            geo_send[t] = tile

    row = lax.broadcasted_iota(jnp.int32, (4 * BLOCK, 256), 0)
    column = lax.broadcasted_iota(jnp.int32, (4 * BLOCK, 256), 1)
    for b in range(SPOKE_DEV // 4):
        wanted = owner_ref[4 * b] * ROWS - REACH + row
        for k in range(1, 4):
            wanted = jnp.where(row >= k * BLOCK, owner_ref[4 * b + k] * ROWS - REACH - k * BLOCK + row, wanted)
        select[b * 4 * BLOCK : (b + 1) * 4 * BLOCK, :] = jnp.where(wanted == column, 1.0, 0.0).astype(BF16)

    def fill(c):
        for p in range(SLOTS):
            stage[pl.ds(p, SPOKE_DEV * BLOCK, stride=SLOTS), :] = dot_nt(
                select[...], kd[p, c * COLS : (c + 1) * COLS, :]
            )
        send[:, :, c * COLS : (c + 1) * COLS] = stage[...].astype(BF16).reshape(SPOKE_DEV, BLOCK * SLOTS, COLS)

    loads[5].wait()
    fill(0)
    fill(1)

    pl.semaphore_wait(barrier, SPOKE_DEV - 1 + COIL_DEV - 1)

    def geo_copy(t):
        return pltpu.make_async_remote_copy(
            geo_send.at[t],
            geo.at[coil, t],
            geo_ssem.at[t],
            geo_rsem.at[t],
            device_id=(coil, geo_dest(t)),
            device_id_type=MESH,
        )

    def value_copy(c, slot, dest):
        rows = (pl.ds(0, EARLY), pl.ds(EARLY, BLOCK * SLOTS - EARLY))[c]
        return pltpu.make_async_remote_copy(
            send.at[dest, rows],
            recv.at[slot, rows],
            val_ssem.at[c, slot],
            val_rsem.at[c, slot],
            device_id=(coil, dest),
            device_id_type=MESH,
        )

    def pass_copy(step):
        return pltpu.make_async_remote_copy(
            geo.at[coil],
            geo.at[coil],
            pass_ssem.at[step],
            pass_rsem.at[step],
            device_id=(lax.rem(coil + step, COIL_DEV), me),
            device_id_type=MESH,
        )

    def pass_arrival(source):
        step = lax.rem(coil - source + COIL_DEV, COIL_DEV)
        return pltpu.make_async_remote_copy(
            geo.at[source],
            geo.at[source],
            pass_ssem.at[step],
            pass_rsem.at[step],
            device_id=(coil_at[1], me),
            device_id_type=MESH,
        )

    @pl.when(coil < CARRY)
    def _():
        for t in range(1, TILES):
            geo_copy(t).start()

    @pl.when((coil > 0) & (coil < CARRY))
    def _():
        geo_copy(0).start()

    @pl.when(coil == 0)
    def _():
        geo[0, 0] = geo_send[0]

    for slot in range(1, SPOKE_DEV):
        value_copy(0, slot, away(slot)).start()
    for zt in (0, 1, 2, 3, 7, 4, 6, 5):
        dz = lax.rem(zt - z + Z_DEV, Z_DEV)
        back = (dz + 3) // 8
        ahead = (dz + 7) // 8 - back
        r = ahead * (2 * dz - 1) + back * (2 * (Z_DEV - dz))
        for dx in (0, 1, 3, 2):
            dest = x_at[dx] + zt

            @pl.when(dest != me)
            def _():
                value_copy(1, dx * Z_DEV + r, dest).start()


    recv[0] = send[me]

    @pl.when(coil < CARRY)
    def _():
        for t in range(1, TILES):
            geo_copy(t).wait_recv()

    @pl.when((coil > 0) & (coil < CARRY))
    def _():
        geo_copy(0).wait_recv()

    @pl.when(coil < CARRY)
    def _():
        for step in range(1, COIL_DEV):
            pass_copy(step).start()

    for source in range(CARRY):

        @pl.when(coil != source)
        def _():
            pass_arrival(source).wait_recv()

    first_row = (owner_ref[me] * ROWS).astype(F32)
    cells = lax.broadcasted_iota(jnp.int32, (8, 256), 1).astype(F32)

    @pl.loop(0, SPOKE_DEV)
    def _(slot):
        group = slot // PER
        member = lax.rem(slot, PER)
        tile = geo[lax.rem(slot, CARRY), slot // CARRY]

        def spread(comp, j):
            lane = comp * 32 + j
            return jnp.broadcast_to(tile[:, lane : lane + 1], (8, 256))

        across, along = [], []
        for j in range(BLOCK):
            start = spread(3, j)
            covered = (cells >= start) & (cells < start + FW)
            across.append(jnp.where(covered, kernel(cells + 0.5 - spread(1, j)), 0.0))
            along.append((spread(0, j)[:, :128], spread(2, j)[:, :128]))
        at = pl.multiple_of(member * 16, 16)
        for g in range(ROWS):
            for i in range(3):
                pair = []
                for j in (2 * (g // 2 + i), 2 * (g // 2 + i) + 1):
                    row, dens = along[j]
                    value = dens * kernel(first_row + (g + 0.5) - row)
                    pair.append(jnp.concatenate([value, value], axis=1) * across[j])
                weights[group, g, pl.ds(i * 16 * PER + at, 16), :] = jnp.concatenate(pair, axis=0).astype(BF16)

    for load in loads[6:]:
        load.wait()

    def arrived(c, q):
        @pl.loop(max(1, q * PER), (q + 1) * PER)
        def _(slot):
            value_copy(c, slot, x_at[1]).wait_recv()

    def folded(i, q, c):
        got = recv[q * PER : (q + 1) * PER, i * 16 : (i + 1) * 16, c * COLS : (c + 1) * COLS].reshape(16 * PER, COLS)
        both = dot_nt(depth_ref[0], got) + dot_nt(depth_ref[1], got)
        fold[:, i * 16 * PER : (i + 1) * 16 * PER] = both.astype(BF16)

    def transform(c, h):
        spectrum = jnp.concatenate(
            [jnp.concatenate([grid[c, g, :64], grid[c, g, 64:]], axis=1) for g in (2 * h, 2 * h + 1)], axis=0
        ).astype(BF16)
        turned = dot(spectrum, column_ref[0]) + dot(spectrum, column_ref[1])
        for g in (2 * h, 2 * h + 1):
            at = (g - 2 * h) * 64
            real, imag = turned[at : at + 64, :256], turned[at : at + 64, 256:]
            images[g, c, 0] = real
            images[g, c, 1] = imag
            mine = real * real + imag * imag
            power[g] = mine if c == 0 else power[g] + mine

    def share(part):
        for h in POWER_PARTS[part]:
            for k in range(COIL_DEV):
                power_send[k, 16 * h : 16 * h + 16] = jnp.concatenate(
                    [power[g, 8 * k : 8 * k + 8] for g in (2 * h, 2 * h + 1)], axis=0
                ).astype(BF16)
        for step in range(1, COIL_DEV):
            power_copy(part, step).start()

    def power_copy(part, step):
        rows = pl.ds(16 * POWER_PARTS[part][0], 16 * len(POWER_PARTS[part]))
        return pltpu.make_async_remote_copy(
            power_send.at[coil_at[step], rows],
            power_recv.at[step, rows],
            pow_ssem.at[part, step],
            pow_rsem.at[part, step],
            device_id=(coil_at[step], me),
            device_id_type=MESH,
        )

    last = PAIRS - 1
    for q in range(GROUPS):
        arrived(0, q)
        for c in range(2):
            for i in range(last):
                folded(i, q, c)
            for g in range(ROWS):
                depth = BAND if g // 2 + 2 < last else BAND - 16 * PER
                at = (g // 2) * 16 * PER
                term = dot(fold[:, at : at + depth], weights[q, g, :depth])
                grid[c, g] = term if q == 0 else grid[c, g] + term
    for h in range(ROWS // 2 - 1):
        transform(0, h)
        transform(1, h)
    share(0)
    for q in range(GROUPS):
        arrived(1, q)
        for c in range(2):
            folded(last, q, c)
            got = fold[:, last * 16 * PER :]
            for g in (ROWS - 2, ROWS - 1):
                grid[c, g] = grid[c, g] + dot(got, weights[q, g, BAND - 16 * PER :])
    for c in range(2):
        transform(c, ROWS // 2 - 1)
    share(1)

    for c in range(2):

        @pl.loop(1, SPOKE_DEV)
        def _(slot):
            value_copy(c, slot, x_at[1]).wait_send()

    @pl.when(coil < CARRY)
    def _():
        for t in range(1, TILES):
            geo_copy(t).wait_send()
        for step in range(1, COIL_DEV):
            pass_copy(step).wait_send()

    @pl.when((coil > 0) & (coil < CARRY))
    def _():
        geo_copy(0).wait_send()

    for part, lines in enumerate(POWER_PARTS):
        for step in range(1, COIL_DEV):
            power_copy(part, step).wait_recv()
        for h in lines:
            rows = pl.ds(16 * h, 16)
            total = power_send[coil, rows].astype(F32)
            for k in range(1, COIL_DEV):
                total = total + power_recv[k, rows].astype(F32)
            combined = jnp.sqrt(total)
            combined_ref[2 * h] = combined[:8]
            combined_ref[2 * h + 1] = combined[8:]

    for part in range(len(POWER_PARTS)):
        for step in range(1, COIL_DEV):
            power_copy(part, step).wait_send()


def written(images, combined, images_out, combined_out, sem):
    copies = [
        pltpu.make_async_copy(images, images_out, sem.at[0]),
        pltpu.make_async_copy(combined, combined_out, sem.at[1]),
    ]
    for copy in copies:
        copy.start()
    for copy in copies:
        copy.wait()


def on_device(kdata, coords, foot_offset, live_count, dcf_table, dcf_index, slab_owner):
    slots, coil_dev, parts, kz, samp = kdata.shape
    kd = kdata.reshape(slots, coil_dev * parts * kz, samp)
    depth = in_two(depth_table(kz))
    column = in_two(column_table(samp))
    vmem = pl.BlockSpec(memory_space=pltpu.VMEM)
    hbm = pl.BlockSpec(memory_space=pltpu.HBM)
    dma = pltpu.SemaphoreType.DMA
    images, combined = pl.pallas_call(
        body,
        out_shape=(
            jax.ShapeDtypeStruct((ROWS, coil_dev, parts, kz, samp), F32),
            jax.ShapeDtypeStruct((ROWS, kz // COIL_DEV, samp), F32),
        ),
        in_specs=[pl.BlockSpec(memory_space=pltpu.SMEM)] + [hbm] * 8,
        out_specs=(vmem, vmem),
        scratch_shapes=[
            pltpu.SMEM(slab_owner.shape, jnp.int32),
            pltpu.SMEM(dcf_table.shape, F32),
            pltpu.VMEM(coords.shape, F32),
            pltpu.VMEM(foot_offset.shape, jnp.int32),
            pltpu.VMEM(dcf_index.shape, jnp.int32),
            pltpu.VMEM(kd.shape, BF16),
            pltpu.VMEM(depth.shape, BF16),
            pltpu.VMEM(column.shape, BF16),
            pltpu.VMEM((SPOKE_DEV * BLOCK, samp), BF16),
            pltpu.VMEM((SPOKE_DEV * BLOCK * SLOTS, COLS), F32),
            pltpu.VMEM((SPOKE_DEV, BLOCK * SLOTS, 2 * COLS), BF16),
            pltpu.VMEM((SPOKE_DEV, BLOCK * SLOTS, 2 * COLS), BF16),
            pltpu.VMEM((TILES, 8, 128), F32),
            pltpu.VMEM((CARRY, TILES, 8, 128), F32),
            pltpu.VMEM((GROUPS, ROWS, BAND, 256), BF16),
            pltpu.VMEM((COLS, PAIRS * 16 * PER), BF16),
            pltpu.VMEM((2, ROWS, COLS, 256), F32),
            pltpu.VMEM((ROWS, kz, samp), F32),
            pltpu.VMEM((COIL_DEV, ROWS * 8, samp), BF16),
            pltpu.VMEM((COIL_DEV, ROWS * 8, samp), BF16),
            dma((8,)),
            dma((TILES,)),
            dma((TILES,)),
            dma((COIL_DEV,)),
            dma((COIL_DEV,)),
            dma((2, SPOKE_DEV)),
            dma((2, SPOKE_DEV)),
            dma((len(POWER_PARTS), COIL_DEV)),
            dma((len(POWER_PARTS), COIL_DEV)),
        ],
        compiler_params=pltpu.CompilerParams(
            collective_id=0, has_side_effects=True, vmem_limit_bytes=24 * 2**20
        ),
    )(
        live_count,
        *(
            pltpu.with_memory_space_constraint(a, pltpu.HBM)
            for a in (slab_owner, dcf_table, coords, foot_offset, dcf_index, kd, depth, column)
        ),
    )
    return pl.pallas_call(
        written,
        out_shape=(
            jax.ShapeDtypeStruct(images.shape, F32),
            jax.ShapeDtypeStruct(combined.shape, F32),
        ),
        in_specs=[hbm] * 2,
        out_specs=(hbm, hbm),
        scratch_shapes=[dma((2,))],
        compiler_params=pltpu.CompilerParams(vmem_limit_bytes=2**20),
    )(images, combined)


def solution(mesh):
    return jax.shard_map(
        on_device,
        mesh=mesh,
        in_specs=(
            P("spoke", "coil", None, None, None),
            P("spoke", None, None),
            P("spoke", None),
            P("spoke"),
            P(),
            P("spoke", None),
            P(),
        ),
        out_specs=(P("spoke", "coil", None, None, None), P("spoke", "coil", None)),
        check_vma=False,
    )
```
